512 devices in a mesh: ep: 8 (over y_lo, x), tp: 8 (over z), dp: 8 (over y_hi, core).
Axes of the slice: x: 4, y: 8 (y_hi: 4, y_lo: 2; y = y_hi * 2 + y_lo), z: 8, core: 2. Of those that a mesh axis runs over, the one named last changes fastest.
Arguments:
- down_weight: bfloat16 [8, 16384, 3072], P('ep', 'tp', 'dp'), may hold values from -130 to 130
- owned_span: int32 [8, 8, 8], replicated, may hold values from 0 to 511, as said below
Outputs:
- saved_spans: bfloat16 [8, 8, 384, 16384], P('ep', 'tp', 'dp')
The draws below stay inside these ranges and needn't reach their ends.
Inputs may be any that keep to these rules, and one draw needn't show every extreme that they name: `owned_span`: block g holds rows (g % 64) * 48 onward of expert g // 64; every block is stored by exactly one device; the block at [i, j, k] has (g % 64) // 8 == k; for each k the experts of the stored blocks form a Latin square over i and j: each expert once for each i and once for each j.
All inputs are finite; a program needn't handle non-finite values.
Results may differ from the reference program's by a relative error of at most 0.001.
Values may be sent and summed in bfloat16 or wider, within the bound.
A program may use at most 64 MiB of HBM per device.

```python
import jax
import jax.numpy as jnp

FF = 16384
EXPERTS = 8
SLAB = 3072
BLOCK_ROWS = 48
N_EP = 8
N_TP = 8
N_DP = 8


def permuted_rows(key, count_rows, width):
    scores = jax.random.randint(key, (count_rows, width), 0, 1 << 20) * width + jnp.arange(width, dtype=jnp.int32)[None, :]
    return jnp.argsort(scores, axis=1).astype(jnp.int32)


def draw_owned_span(key, part):
    key_list = jax.random.split(jax.random.fold_in(key, 23), 4)
    per_expert = N_TP * N_DP
    row_perm = permuted_rows(key_list[0], N_DP, N_EP)
    col_perm = permuted_rows(key_list[1], N_DP, N_TP)
    relabel = permuted_rows(key_list[2], N_DP, N_EP)
    block_perm = permuted_rows(key_list[3], N_DP * N_EP, N_TP).reshape(N_DP, N_EP, N_TP)
    summed = (row_perm[:, :, None] + col_perm[:, None, :]) % N_EP
    latin_square = jnp.take_along_axis(relabel[:, :, None], summed.reshape(N_DP, N_EP * N_TP, 1), axis=1).reshape(N_DP, N_EP, N_TP)
    replica_ids = jnp.arange(N_DP, dtype=jnp.int32)[:, None, None] + jnp.zeros((N_DP, N_EP, N_TP), jnp.int32)
    ep_ids = jnp.arange(N_EP, dtype=jnp.int32)[None, :, None] + jnp.zeros((N_DP, N_EP, N_TP), jnp.int32)
    within = replica_ids * N_TP + block_perm[replica_ids, latin_square, ep_ids]
    global_ids = latin_square * per_expert + within
    return jnp.transpose(global_ids, (1, 2, 0)).astype(jnp.int32)


def draw_down_weight(key, part):
    key_list = jax.random.split(jax.random.fold_in(key, 11), 3)
    base_draw = jnp.clip(jax.random.normal(key_list[0], (EXPERTS, FF, SLAB), jnp.float32), -4.0, 4.0)
    spread = 1.15
    row_scale = jnp.exp(jax.random.uniform(key_list[1], (SLAB,), jnp.float32, -spread, spread))
    col_scale = jnp.exp(jax.random.uniform(key_list[2], (FF,), jnp.float32, -spread, spread))
    expert_scale = jnp.power(3.0, jnp.arange(EXPERTS, dtype=jnp.float32) / max(EXPERTS - 1, 1))
    values = base_draw * expert_scale[:, None, None] * col_scale[None, :, None] * row_scale[None, None, :]
    return values.astype(jnp.bfloat16)


def setup_inputs(seed: int = 0) -> dict:
    keys = jax.random.split(jax.random.key(seed), 3)
    down_weight = draw_down_weight(jax.random.fold_in(keys[2], 71), 0)
    owned_span = draw_owned_span(jax.random.fold_in(keys[2], 71), 0)
    return {"down_weight": down_weight, "owned_span": owned_span}


def reference(down_weight, owned_span):
    per_expert = N_TP * N_DP
    saved_rows = jnp.transpose(down_weight, (0, 2, 1)).reshape(EXPERTS * per_expert, BLOCK_ROWS, FF)
    owner_list = owned_span.reshape(-1).astype(jnp.int32)
    picked = jnp.take(saved_rows, owner_list, axis=0)
    saved_spans = picked.reshape(N_EP, N_TP, N_DP * BLOCK_ROWS, FF)
    return saved_spans
```

```python
import functools

import jax
import jax.numpy as jnp
from jax import lax
from jax.experimental import pallas as pl
from jax.experimental.pallas import tpu as pltpu
from jax.sharding import PartitionSpec as P

MESH = pl.DeviceIdType.MESH
HIDDEN = 2048
ROWS = 384
SPANS = 8
BLOCK = 48
CHUNKS = (128, 128, 256, 512, 512, 512)
STARTS = tuple(sum(CHUNKS[:n]) for n in range(len(CHUNKS)))
EP_STEPS = ((1, 2), (1, 1), (1, 3), (0, 2), (1, 0), (0, 1), (0, 3))
TP_STEPS = (1, 7, 2, 6, 3, 5, 4)


def ep_member(index, step):
    half, along = lax.div(index, 4), lax.rem(index, 4)
    return lax.rem(half + step[0], 2) * 4 + lax.rem(along + step[1], 4)


def kernel(weight, span, out, x_in, table, turned, *rest):
    count = len(CHUNKS)
    send_one, recv_one, send_two = rest[:count], rest[count : 2 * count], rest[2 * count : 3 * count]
    in_sem, table_sem, ss_one, rs_one, ss_two, rs_two = rest[3 * count :]
    my_ep = lax.axis_index("ep")
    my_tp = lax.axis_index("tp")
    my_dp = lax.axis_index("dp")

    barrier = pltpu.get_barrier_semaphore()
    for step in EP_STEPS:
        pl.semaphore_signal(barrier, inc=1, device_id={"ep": ep_member(my_ep, step)}, device_id_type=MESH)
    for step in TP_STEPS:
        pl.semaphore_signal(barrier, inc=1, device_id={"tp": lax.rem(my_tp + step, 8)}, device_id_type=MESH)

    table_copy = pltpu.make_async_copy(span, table, table_sem)
    table_copy.start()
    loads = []
    for c, (start, width) in enumerate(zip(STARTS, CHUNKS)):
        load = pltpu.make_async_copy(weight.at[0, pl.ds(start, width)], x_in.at[pl.ds(start, width)], in_sem.at[c])
        load.start()
        loads.append(load)
    table_copy.wait()

    def span_for(member):
        found = 0
        for j in range(8):
            owned = table[member, j, my_dp]
            mine = 1 - lax.min(lax.abs(lax.div(owned, 64) - my_ep), 1)
            found += mine * lax.rem(owned, SPANS)
        return found

    members = [my_ep] + [ep_member(my_ep, step) for step in EP_STEPS]
    spans = [span_for(member) for member in members]
    targets = [my_tp] + [lax.rem(my_tp + step, 8) for step in TP_STEPS]
    experts = [lax.div(table[my_ep, target, my_dp], 64) for target in targets]

    sends_one, sends_two = [], []
    for c, (start, width) in enumerate(zip(STARTS, CHUNKS)):
        loads[c].wait()
        turned[:, :, pl.ds(start, width)] = jnp.transpose(x_in[pl.ds(start, width), :]).reshape(SPANS, BLOCK, width)
        for n, member in enumerate(members):
            block = turned[spans[n], :, pl.ds(start, width)]
            if n == 0:
                recv_one[c][my_ep] = block
            else:
                send_one[c][n - 1] = block
        if c == 0:
            pl.semaphore_wait(barrier, 14)
        for n, member in enumerate(members[1:]):
            copy = pltpu.make_async_remote_copy(
                src_ref=send_one[c].at[n],
                dst_ref=recv_one[c].at[my_ep],
                send_sem=ss_one.at[c, n],
                recv_sem=rs_one.at[c, n],
                device_id={"ep": member},
                device_id_type=MESH,
            )
            copy.start()
            sends_one.append(copy)

    for c, (start, width) in enumerate(zip(STARTS, CHUNKS)):
        for n in range(7):
            sends_one[c * 7 + n].wait_recv()
        for n, target in enumerate(targets):
            block = recv_one[c][experts[n]]
            if n == 0:
                mine = pl.multiple_of(my_tp * HIDDEN + start, 128)
                out[:, pl.ds(mine, width)] = block
            else:
                send_two[c][n - 1] = block
        for n, target in enumerate(targets[1:]):
            copy = pltpu.make_async_remote_copy(
                src_ref=send_two[c].at[n],
                dst_ref=out.at[:, pl.ds(pl.multiple_of(my_tp * HIDDEN + start, 128), width)],
                send_sem=ss_two.at[c, n],
                recv_sem=rs_two.at[c, n],
                device_id={"tp": target},
                device_id_type=MESH,
            )
            copy.start()
            sends_two.append(copy)

    for copy in sends_one:
        copy.wait_send()
    for copy in sends_two:
        copy.wait()


def local(down_weight, owned_span):
    count = len(CHUNKS)
    slots = lambda number: [pltpu.VMEM((number, BLOCK, width), jnp.bfloat16) for width in CHUNKS]
    saved = pl.pallas_call(
        kernel,
        out_shape=pltpu.VMEM((BLOCK, 8 * HIDDEN), jnp.bfloat16),
        in_specs=[pl.BlockSpec(memory_space=pltpu.HBM), pl.BlockSpec(memory_space=pltpu.HBM)],
        out_specs=pl.BlockSpec(memory_space=pltpu.VMEM),
        scratch_shapes=[
            pltpu.VMEM((HIDDEN, ROWS), jnp.bfloat16),
            pltpu.SMEM((8, 8, 8), jnp.int32),
            pltpu.VMEM((SPANS, BLOCK, HIDDEN), jnp.bfloat16),
            *slots(7),
            *slots(8),
            *slots(7),
            pltpu.SemaphoreType.DMA((count,)),
            pltpu.SemaphoreType.DMA,
            pltpu.SemaphoreType.DMA((count, 7)),
            pltpu.SemaphoreType.DMA((count, 7)),
            pltpu.SemaphoreType.DMA((count, 7)),
            pltpu.SemaphoreType.DMA((count, 7)),
        ],
        compiler_params=pltpu.CompilerParams(collective_id=0, has_side_effects=True, vmem_limit_bytes=60 << 20),
    )(down_weight, owned_span)
    return saved[None, None]


def solution(mesh):
    return jax.shard_map(
        local,
        mesh=mesh,
        in_specs=(P("ep", "tp", "dp"), P()),
        out_specs=P("ep", "tp", "dp", None),
        check_vma=False,
    )
```

```python
import jax
import jax.numpy as jnp
from jax import lax
from jax.experimental import pallas as pl
from jax.experimental.pallas import tpu as pltpu
from jax.sharding import PartitionSpec as P

LOGICAL = pl.DeviceIdType.LOGICAL
HIDDEN = 2048
ROWS = 384
SPANS = 8
BLOCK = 48
FIRST = 384
CHUNKS = (256, 384, 512, 512)
EARLY = 1
ORDERS = ("asc",) * 5
SCATTER = 1
STARTS = tuple(FIRST + sum(CHUNKS[:n]) for n in range(len(CHUNKS)))
EP_STEPS = ((1, 2), (1, 1), (1, 3), (0, 2), (1, 0), (0, 1), (0, 3))
TP_STEPS = (1, 7, 2, 6, 3, 5, 4)


def ep_member(index, step):
    return ((index + 4 * step[0]) & 4) + ((index + step[1]) & 3)


def others(index):
    return [n + ((n - index + 8) >> 3) for n in range(7)]


def kernel(weight, span, out, x_in, table, turned, z_send, z_recv, z_mid, z_last, *rest):
    count = len(CHUNKS)
    send_one, recv_one, send_two = rest[:count], rest[count : 2 * count], rest[2 * count : 3 * count]
    in_sem, table_sem, ss_one, rs_one, ss_two, rs_two, ss_z, rs_z = rest[3 * count :]
    my_ep = lax.axis_index("ep")
    my_tp = lax.axis_index("tp")
    my_dp = lax.axis_index("dp")

    members = [ep_member(my_ep, step) for step in EP_STEPS]
    ep_ids = [member * 64 + my_tp * 8 + my_dp for member in members]
    tp_orders = {"near": [(my_tp + step) & 7 for step in TP_STEPS], "asc": others(my_tp)}
    sources = tp_orders["near"]

    def tp_id(target):
        return my_ep * 64 + target * 8 + my_dp

    barrier = pltpu.get_barrier_semaphore()
    for other in [tp_id(target) for target in tp_orders["near"][::-1]] + ep_ids:
        pl.semaphore_signal(barrier, inc=1, device_id=other, device_id_type=LOGICAL)

    table_copy = pltpu.make_async_copy(span, table, table_sem)
    table_copy.start()
    parts = [(0, FIRST)] + list(zip(STARTS, CHUNKS))
    loads = []
    for c, (start, width) in enumerate(parts):
        load = pltpu.make_async_copy(weight.at[0, pl.ds(start, width)], x_in.at[pl.ds(start, width)], in_sem.at[c])
        load.start()
        loads.append(load)
    table_copy.wait()

    def expert_of(member, target):
        return table[member, target, my_dp] >> 6

    def span_if_mine(member, target):
        owned = table[member, target, my_dp]
        return (1 - lax.min(lax.abs((owned >> 6) - my_ep), 1)) * (owned & 7)

    def span_for_member(member):
        return sum(span_if_mine(member, j) for j in range(8))

    def span_for_target(target):
        return sum(span_if_mine(i, target) for i in range(8))

    def turn(part):
        start, width = parts[part]
        loads[part].wait()
        turned[:, :, pl.ds(start, width)] = jnp.transpose(x_in[pl.ds(start, width), :]).reshape(SPANS, BLOCK, width)

    def remote(src, dst, send_sem, recv_sem, other):
        return pltpu.make_async_remote_copy(
            src_ref=src, dst_ref=dst, send_sem=send_sem, recv_sem=recv_sem, device_id=other, device_id_type=LOGICAL
        )

    started, awaited = [], []

    turn(0)
    z_targets = tp_orders[ORDERS[0]]
    z_recv[my_tp] = turned[span_for_target(my_tp), :, pl.ds(0, FIRST)]
    for n, target in enumerate(z_targets):
        z_send[n] = turned[span_for_target(target), :, pl.ds(0, FIRST)]

    spans = [span_for_member(member) for member in [my_ep] + members]

    def stage(c):
        turn(c + 1)
        start, width = STARTS[c], CHUNKS[c]
        recv_one[c][my_ep] = turned[spans[0], :, pl.ds(start, width)]
        for n in range(7):
            send_one[c][n] = turned[spans[n + 1], :, pl.ds(start, width)]

    for c in range(EARLY):
        stage(c)
    pl.semaphore_wait(barrier, 14)

    for n, target in enumerate(z_targets):
        copy = remote(z_send.at[n], z_recv.at[my_tp], ss_z.at[0, n], rs_z.at[0, my_tp], tp_id(target))
        copy.start()
        started.append(copy)

    one = []
    for c in range(count):
        if c >= EARLY:
            stage(c)
        for n, other in enumerate(ep_ids):
            copy = remote(send_one[c].at[n], recv_one[c].at[my_ep], ss_one.at[c, n], rs_one.at[c, n], other)
            copy.start()
            started.append(copy)
            one.append(copy)

    def columns(shard, start, width):
        return pl.ds(pl.multiple_of(shard * HIDDEN + start, 128), width)

    for c in range(count):
        start, width = STARTS[c], CHUNKS[c]
        for n in range(7):
            one[c * 7 + n].wait_recv()
        targets = tp_orders[ORDERS[c + 1]]
        for n, target in enumerate(targets):
            send_two[c][n] = recv_one[c][expert_of(my_ep, target)]
        for n, target in enumerate(targets):
            mine = out.at[:, columns(my_tp, start, width)]
            copy = remote(send_two[c].at[n], mine, ss_two.at[c, n], rs_two.at[c, my_tp], tp_id(target))
            copy.start()
            started.append(copy)
        out[:, columns(my_tp, start, width)] = recv_one[c][expert_of(my_ep, my_tp)]
        for source in sources:
            theirs = out.at[:, columns(source, start, width)]
            awaited.append(remote(send_two[c].at[0], theirs, ss_two.at[c, 0], rs_two.at[c, source], tp_id(source)))

        if c == SCATTER:
            for source in sources:
                remote(z_send.at[0], z_recv.at[source], ss_z.at[0, 0], rs_z.at[0, source], tp_id(source)).wait_recv()
            for n, member in enumerate(members):
                copy = remote(z_recv.at[member], z_mid.at[my_ep], ss_z.at[1, n], rs_z.at[1, n], ep_ids[n])
                copy.start()
                started.append(copy)
            z_mid[my_ep] = z_recv[my_ep]

    for n, member in enumerate(members):
        remote(z_recv.at[0], z_mid.at[member], ss_z.at[1, n], rs_z.at[1, n], ep_ids[n]).wait_recv()
    for n, member in enumerate(members):
        z_last[n] = z_mid[expert_of(member, my_tp)]
    for n, member in enumerate(members):
        mine = out.at[:, columns(my_ep, 0, FIRST)]
        copy = remote(z_last.at[n], mine, ss_z.at[2, n], rs_z.at[2, n], ep_ids[n])
        copy.start()
        started.append(copy)
    out[:, columns(my_ep, 0, FIRST)] = z_mid[expert_of(my_ep, my_tp)]
    for n, member in enumerate(members):
        theirs = out.at[:, columns(member, 0, FIRST)]
        awaited.append(remote(z_last.at[n], theirs, ss_z.at[2, n], rs_z.at[2, n], ep_ids[n]))

    for copy in awaited:
        copy.wait_recv()
    for copy in started:
        copy.wait_send()


def local(down_weight, owned_span):
    count = len(CHUNKS)

    def slots(number, width):
        return pltpu.VMEM((number, BLOCK, width), jnp.bfloat16)

    saved = pl.pallas_call(
        kernel,
        out_shape=pltpu.VMEM((BLOCK, 8 * HIDDEN), jnp.bfloat16),
        in_specs=[pl.BlockSpec(memory_space=pltpu.HBM), pl.BlockSpec(memory_space=pltpu.HBM)],
        out_specs=pl.BlockSpec(memory_space=pltpu.VMEM),
        scratch_shapes=[
            pltpu.VMEM((HIDDEN, ROWS), jnp.bfloat16),
            pltpu.SMEM((8, 8, 8), jnp.int32),
            pltpu.VMEM((SPANS, BLOCK, HIDDEN), jnp.bfloat16),
            slots(7, FIRST),
            slots(8, FIRST),
            slots(8, FIRST),
            slots(7, FIRST),
            *[slots(7, width) for width in CHUNKS],
            *[slots(8, width) for width in CHUNKS],
            *[slots(7, width) for width in CHUNKS],
            pltpu.SemaphoreType.DMA((count + 1,)),
            pltpu.SemaphoreType.DMA,
            pltpu.SemaphoreType.DMA((count, 7)),
            pltpu.SemaphoreType.DMA((count, 7)),
            pltpu.SemaphoreType.DMA((count, 7)),
            pltpu.SemaphoreType.DMA((count, 8)),
            pltpu.SemaphoreType.DMA((3, 7)),
            pltpu.SemaphoreType.DMA((3, 8)),
        ],
        compiler_params=pltpu.CompilerParams(collective_id=0, has_side_effects=True, vmem_limit_bytes=60 << 20),
    )(down_weight, owned_span)
    return saved[None, None]


def solution(mesh):
    return jax.shard_map(
        local,
        mesh=mesh,
        in_specs=(P("ep", "tp", "dp"), P()),
        out_specs=P("ep", "tp", "dp", None),
        check_vma=False,
    )
```

```python
import jax
import jax.numpy as jnp
from jax import lax
from jax.experimental import pallas as pl
from jax.experimental.pallas import tpu as pltpu
from jax.sharding import PartitionSpec as P

LOGICAL = pl.DeviceIdType.LOGICAL
HIDDEN = 2048
ROWS = 384
SPANS = 8
BLOCK = 48
FIRST = 640
CHUNKS = (512, 896)
EARLY = 1
LOW = (0, 1, 2, 3, 4, 5, 6, 7)
ORDERS = (None,) * len(CHUNKS) + (LOW,)
SCATTER = 0
STARTS = tuple(FIRST + sum(CHUNKS[:n]) for n in range(len(CHUNKS)))
EP_STEPS = ((1, 2), (1, 1), (1, 3), (0, 2), (1, 0), (0, 1), (0, 3))
TP_STEPS = (1, 7, 2, 6, 3, 5, 4)


def ep_member(index, step):
    return ((index + 4 * step[0]) & 4) + ((index + step[1]) & 3)


def others(index, order):
    place = sum(n * (1 - lax.min(lax.abs(index - target), 1)) for n, target in enumerate(order))
    return [order[n] + ((n - place + 8) >> 3) * (order[n + 1] - order[n]) for n in range(7)]


def kernel(weight, span, out, x_in, table, turned, z_send, z_recv, z_mid, z_last, *rest):
    count = len(CHUNKS)
    send_one, recv_one, send_two = rest[:count], rest[count : 2 * count], rest[2 * count : 3 * count]
    in_sem, table_sem, ss_one, rs_one, ss_two, rs_two, ss_z, rs_z = rest[3 * count :]
    my_ep = lax.axis_index("ep")
    my_tp = lax.axis_index("tp")
    my_dp = lax.axis_index("dp")

    members = [ep_member(my_ep, step) for step in EP_STEPS]
    ep_ids = [member * 64 + my_tp * 8 + my_dp for member in members]
    sources = [(my_tp + step) & 7 for step in TP_STEPS]
    tp_orders = [sources if order is None else others(my_tp, order) for order in ORDERS]

    def tp_id(target):
        return my_ep * 64 + target * 8 + my_dp

    barrier = pltpu.get_barrier_semaphore()
    for other in [tp_id(target) for target in sources[::-1]] + ep_ids:
        pl.semaphore_signal(barrier, inc=1, device_id=other, device_id_type=LOGICAL)

    table_copy = pltpu.make_async_copy(span, table, table_sem)
    table_copy.start()
    parts = [(0, FIRST)] + list(zip(STARTS, CHUNKS))
    loads = []
    for c, (start, width) in enumerate(parts):
        load = pltpu.make_async_copy(weight.at[0, pl.ds(start, width)], x_in.at[pl.ds(start, width)], in_sem.at[c])
        load.start()
        loads.append(load)
    table_copy.wait()

    def expert_of(member, target):
        return table[member, target, my_dp] >> 6

    def span_if_mine(member, target):
        owned = table[member, target, my_dp]
        return (1 - lax.min(lax.abs((owned >> 6) - my_ep), 1)) * (owned & 7)

    def span_for_member(member):
        return sum(span_if_mine(member, j) for j in range(8))

    def span_for_target(target):
        return sum(span_if_mine(i, target) for i in range(8))

    def turn(part):
        start, width = parts[part]
        loads[part].wait()
        turned[:, :, pl.ds(start, width)] = jnp.transpose(x_in[pl.ds(start, width), :]).reshape(SPANS, BLOCK, width)

    def remote(src, dst, send_sem, recv_sem, other):
        return pltpu.make_async_remote_copy(
            src_ref=src, dst_ref=dst, send_sem=send_sem, recv_sem=recv_sem, device_id=other, device_id_type=LOGICAL
        )

    started, awaited = [], []

    turn(0)
    z_targets = tp_orders[0]
    z_recv[my_tp] = turned[span_for_target(my_tp), :, pl.ds(0, FIRST)]
    for n, target in enumerate(z_targets):
        z_send[n] = turned[span_for_target(target), :, pl.ds(0, FIRST)]

    spans = [span_for_member(member) for member in [my_ep] + members]

    def stage(c):
        turn(c + 1)
        start, width = STARTS[c], CHUNKS[c]
        recv_one[c][my_ep] = turned[spans[0], :, pl.ds(start, width)]
        for n in range(7):
            send_one[c][n] = turned[spans[n + 1], :, pl.ds(start, width)]

    for c in range(EARLY):
        stage(c)
    pl.semaphore_wait(barrier, 14)

    for n, target in enumerate(z_targets):
        copy = remote(z_send.at[n], z_recv.at[my_tp], ss_z.at[0, n], rs_z.at[0, my_tp], tp_id(target))
        copy.start()
        started.append(copy)

    one = []
    for c in range(count):
        if c >= EARLY:
            stage(c)
        for n, other in enumerate(ep_ids):
            copy = remote(send_one[c].at[n], recv_one[c].at[my_ep], ss_one.at[c, n], rs_one.at[c, n], other)
            copy.start()
            started.append(copy)
            one.append(copy)

    def columns(shard, start, width):
        return pl.ds(pl.multiple_of(shard * HIDDEN + start, 128), width)

    for c in range(count):
        start, width = STARTS[c], CHUNKS[c]
        for n in range(7):
            one[c * 7 + n].wait_recv()
        targets = tp_orders[c + 1]
        for n, target in enumerate(targets):
            send_two[c][n] = recv_one[c][expert_of(my_ep, target)]
        for n, target in enumerate(targets):
            mine = out.at[:, columns(my_tp, start, width)]
            copy = remote(send_two[c].at[n], mine, ss_two.at[c, n], rs_two.at[c, my_tp], tp_id(target))
            copy.start()
            started.append(copy)
        out[:, columns(my_tp, start, width)] = recv_one[c][expert_of(my_ep, my_tp)]
        for source in sources:
            theirs = out.at[:, columns(source, start, width)]
            awaited.append(remote(send_two[c].at[0], theirs, ss_two.at[c, 0], rs_two.at[c, source], tp_id(source)))

        if c == SCATTER:
            for source in sources:
                remote(z_send.at[0], z_recv.at[source], ss_z.at[0, 0], rs_z.at[0, source], tp_id(source)).wait_recv()
            for n, member in enumerate(members):
                copy = remote(z_recv.at[member], z_mid.at[my_ep], ss_z.at[1, n], rs_z.at[1, n], ep_ids[n])
                copy.start()
                started.append(copy)
            z_mid[my_ep] = z_recv[my_ep]

    for n, member in enumerate(members):
        remote(z_recv.at[0], z_mid.at[member], ss_z.at[1, n], rs_z.at[1, n], ep_ids[n]).wait_recv()
    for n, member in enumerate(members):
        z_last[n] = z_mid[expert_of(member, my_tp)]
    for n, member in enumerate(members):
        mine = out.at[:, columns(my_ep, 0, FIRST)]
        copy = remote(z_last.at[n], mine, ss_z.at[2, n], rs_z.at[2, n], ep_ids[n])
        copy.start()
        started.append(copy)
    out[:, columns(my_ep, 0, FIRST)] = z_mid[expert_of(my_ep, my_tp)]
    for n, member in enumerate(members):
        theirs = out.at[:, columns(member, 0, FIRST)]
        awaited.append(remote(z_last.at[n], theirs, ss_z.at[2, n], rs_z.at[2, n], ep_ids[n]))

    for copy in awaited:
        copy.wait_recv()
    for copy in started:
        copy.wait_send()


def local(down_weight, owned_span):
    count = len(CHUNKS)

    def slots(number, width):
        return pltpu.VMEM((number, BLOCK, width), jnp.bfloat16)

    saved = pl.pallas_call(
        kernel,
        out_shape=pltpu.VMEM((BLOCK, 8 * HIDDEN), jnp.bfloat16),
        in_specs=[pl.BlockSpec(memory_space=pltpu.HBM), pl.BlockSpec(memory_space=pltpu.HBM)],
        out_specs=pl.BlockSpec(memory_space=pltpu.VMEM),
        scratch_shapes=[
            pltpu.VMEM((HIDDEN, ROWS), jnp.bfloat16),
            pltpu.SMEM((8, 8, 8), jnp.int32),
            pltpu.VMEM((SPANS, BLOCK, HIDDEN), jnp.bfloat16),
            slots(7, FIRST),
            slots(8, FIRST),
            slots(8, FIRST),
            slots(7, FIRST),
            *[slots(7, width) for width in CHUNKS],
            *[slots(8, width) for width in CHUNKS],
            *[slots(7, width) for width in CHUNKS],
            pltpu.SemaphoreType.DMA((count + 1,)),
            pltpu.SemaphoreType.DMA,
            pltpu.SemaphoreType.DMA((count, 7)),
            pltpu.SemaphoreType.DMA((count, 7)),
            pltpu.SemaphoreType.DMA((count, 7)),
            pltpu.SemaphoreType.DMA((count, 8)),
            pltpu.SemaphoreType.DMA((3, 7)),
            pltpu.SemaphoreType.DMA((3, 8)),
        ],
        compiler_params=pltpu.CompilerParams(collective_id=0, has_side_effects=True, vmem_limit_bytes=60 << 20),
    )(down_weight, owned_span)
    return saved[None, None]


def solution(mesh):
    return jax.shard_map(
        local,
        mesh=mesh,
        in_specs=(P("ep", "tp", "dp"), P()),
        out_specs=P("ep", "tp", "dp", None),
        check_vma=False,
    )
```

```python
import jax
import jax.numpy as jnp
from jax import lax
from jax.experimental import pallas as pl
from jax.experimental.pallas import tpu as pltpu
from jax.sharding import PartitionSpec as P

LOGICAL = pl.DeviceIdType.LOGICAL
HIDDEN = 2048
ROWS = 384
SPANS = 8
BLOCK = 48
FIRST = 640
CHUNKS = (512, 896)
EARLY = 1
LOW = (0, 1, 2, 3, 4, 5, 6, 7)
ORDERS = (None,) * len(CHUNKS) + (LOW,)
SCATTER = 0
STARTS = tuple(FIRST + sum(CHUNKS[:n]) for n in range(len(CHUNKS)))
EP_STEPS = ((1, 2), (1, 1), (1, 3), (0, 2), (1, 0), (0, 1), (0, 3))
TP_STEPS = (1, 7, 2, 6, 3, 5, 4)


def ep_member(index, step):
    return ((index + 4 * step[0]) & 4) + ((index + step[1]) & 3)


def others(index, order):
    place = sum(n * (1 - lax.min(lax.abs(index - target), 1)) for n, target in enumerate(order))
    return [order[n] + ((n - place + 8) >> 3) * (order[n + 1] - order[n]) for n in range(7)]


def kernel(weight, span, out, x_in, table, turned, z_send, z_recv, z_mid, z_last, *rest):
    count = len(CHUNKS)
    send_one, recv_one, send_two = rest[:count], rest[count : 2 * count], rest[2 * count : 3 * count]
    in_sem, table_sem, ss_one, rs_one, ss_two, rs_two, ss_z, rs_z = rest[3 * count :]
    my_ep = lax.axis_index("ep")
    my_tp = lax.axis_index("tp")
    my_dp = lax.axis_index("dp")

    def tp_id(target):
        return my_ep * 64 + target * 8 + my_dp

    sources = [(my_tp + step) & 7 for step in TP_STEPS]
    members = [ep_member(my_ep, step) for step in EP_STEPS]
    ep_ids = [member * 64 + my_tp * 8 + my_dp for member in members]
    barrier = pltpu.get_barrier_semaphore()
    for other in [tp_id(target) for target in sources[::-1]] + ep_ids:
        pl.semaphore_signal(barrier, inc=1, device_id=other, device_id_type=LOGICAL)

    table_copy = pltpu.make_async_copy(span, table, table_sem)
    table_copy.start()
    parts = [(0, FIRST)] + list(zip(STARTS, CHUNKS))
    loads = []
    for c, (start, width) in enumerate(parts):
        load = pltpu.make_async_copy(weight.at[0, pl.ds(start, width)], x_in.at[pl.ds(start, width)], in_sem.at[c])
        load.start()
        loads.append(load)

    tp_orders = [sources if order is None else others(my_tp, order) for order in ORDERS]

    def expert_of(member, target):
        return table[member, target, my_dp] >> 6

    def span_if_mine(member, target):
        owned = table[member, target, my_dp]
        return (1 - lax.min(lax.abs((owned >> 6) - my_ep), 1)) * (owned & 7)

    def span_for_member(member):
        return sum(span_if_mine(member, j) for j in range(8))

    def span_for_target(target):
        return sum(span_if_mine(i, target) for i in range(8))

    def turn(part):
        start, width = parts[part]
        loads[part].wait()
        turned[:, :, pl.ds(start, width)] = jnp.transpose(x_in[pl.ds(start, width), :]).reshape(SPANS, BLOCK, width)

    def remote(src, dst, send_sem, recv_sem, other):
        return pltpu.make_async_remote_copy(
            src_ref=src, dst_ref=dst, send_sem=send_sem, recv_sem=recv_sem, device_id=other, device_id_type=LOGICAL
        )

    def group_wait(sem, ref):
        pltpu.make_async_copy(ref, ref, sem).wait()

    turn(0)
    table_copy.wait()
    z_targets = tp_orders[0]
    z_recv[my_tp] = turned[span_for_target(my_tp), :, pl.ds(0, FIRST)]
    for n, target in enumerate(z_targets):
        z_send[n] = turned[span_for_target(target), :, pl.ds(0, FIRST)]

    spans = [span_for_member(member) for member in [my_ep] + members]

    def stage(c):
        turn(c + 1)
        start, width = STARTS[c], CHUNKS[c]
        recv_one[c][my_ep] = turned[spans[0], :, pl.ds(start, width)]
        for n in range(7):
            send_one[c][n] = turned[spans[n + 1], :, pl.ds(start, width)]

    for c in range(EARLY):
        stage(c)
    pl.semaphore_wait(barrier, 14)

    for n, target in enumerate(z_targets):
        remote(z_send.at[n], z_recv.at[my_tp], ss_z.at[0], rs_z.at[0], tp_id(target)).start()

    for c in range(count):
        if c >= EARLY:
            stage(c)
        for n, other in enumerate(ep_ids):
            remote(send_one[c].at[n], recv_one[c].at[my_ep], ss_one.at[c], rs_one.at[c], other).start()

    def columns(shard, start, width):
        return pl.ds(pl.multiple_of(shard * HIDDEN + start, 128), width)

    for c in range(count):
        start, width = STARTS[c], CHUNKS[c]
        group_wait(rs_one.at[c], recv_one[c].at[pl.ds(0, 7)])
        targets = tp_orders[c + 1]
        for n, target in enumerate(targets):
            send_two[c][n] = recv_one[c][expert_of(my_ep, target)]
        for n, target in enumerate(targets):
            mine = out.at[:, columns(my_tp, start, width)]
            remote(send_two[c].at[n], mine, ss_two.at[c], rs_two.at[c], tp_id(target)).start()
        out[:, columns(my_tp, start, width)] = recv_one[c][expert_of(my_ep, my_tp)]

        if c == SCATTER:
            group_wait(rs_z.at[0], z_recv.at[pl.ds(0, 7)])
            for n, member in enumerate(members):
                remote(z_recv.at[member], z_mid.at[my_ep], ss_z.at[1], rs_z.at[1], ep_ids[n]).start()
            z_mid[my_ep] = z_recv[my_ep]

    group_wait(rs_z.at[1], z_mid.at[pl.ds(0, 7)])
    for n, member in enumerate(members):
        z_last[n] = z_mid[expert_of(member, my_tp)]
    for n, member in enumerate(members):
        mine = out.at[:, columns(my_ep, 0, FIRST)]
        remote(z_last.at[n], mine, ss_z.at[2], rs_z.at[2], ep_ids[n]).start()
    out[:, columns(my_ep, 0, FIRST)] = z_mid[expert_of(my_ep, my_tp)]

    group_wait(ss_z.at[0], z_send)
    group_wait(ss_z.at[1], z_recv.at[pl.ds(0, 7)])
    for c in range(count):
        group_wait(ss_one.at[c], send_one[c])
    group_wait(ss_z.at[2], z_last)
    group_wait(rs_z.at[2], out.at[:, pl.ds(0, 7 * FIRST)])
    for c, width in enumerate(CHUNKS):
        group_wait(ss_two.at[c], send_two[c])
        group_wait(rs_two.at[c], out.at[:, pl.ds(0, 7 * width)])


def local(down_weight, owned_span):
    count = len(CHUNKS)

    def slots(number, width):
        return pltpu.VMEM((number, BLOCK, width), jnp.bfloat16)

    saved = pl.pallas_call(
        kernel,
        out_shape=pltpu.VMEM((BLOCK, 8 * HIDDEN), jnp.bfloat16),
        in_specs=[pl.BlockSpec(memory_space=pltpu.HBM), pl.BlockSpec(memory_space=pltpu.HBM)],
        out_specs=pl.BlockSpec(memory_space=pltpu.VMEM),
        scratch_shapes=[
            pltpu.VMEM((HIDDEN, ROWS), jnp.bfloat16),
            pltpu.SMEM((8, 8, 8), jnp.int32),
            pltpu.VMEM((SPANS, BLOCK, HIDDEN), jnp.bfloat16),
            slots(7, FIRST),
            slots(8, FIRST),
            slots(8, FIRST),
            slots(7, FIRST),
            *[slots(7, width) for width in CHUNKS],
            *[slots(8, width) for width in CHUNKS],
            *[slots(7, width) for width in CHUNKS],
            pltpu.SemaphoreType.DMA((count + 1,)),
            pltpu.SemaphoreType.DMA,
            pltpu.SemaphoreType.DMA((count,)),
            pltpu.SemaphoreType.DMA((count,)),
            pltpu.SemaphoreType.DMA((count,)),
            pltpu.SemaphoreType.DMA((count,)),
            pltpu.SemaphoreType.DMA((3,)),
            pltpu.SemaphoreType.DMA((3,)),
        ],
        compiler_params=pltpu.CompilerParams(collective_id=0, has_side_effects=True, vmem_limit_bytes=60 << 20),
    )(down_weight, owned_span)
    return saved[None, None]


def solution(mesh):
    return jax.shard_map(
        local,
        mesh=mesh,
        in_specs=(P("ep", "tp", "dp"), P()),
        out_specs=P("ep", "tp", "dp", None),
        check_vma=False,
    )
```
